16 devices in a mesh: dp: 2 (over z), cp: 8 (over y, x, core).
Axes of the slice: x: 2, y: 2, z: 2, core: 2. Of those that a mesh axis runs over, the one named last changes fastest.
Arguments:
- x: bfloat16 [4096, 5376], P(('dp', 'cp')), parts along dimension 0
- wq: bfloat16 [6, 5376, 32, 128], replicated
- wk: bfloat16 [6, 5376, 16, 128], replicated
- wv: bfloat16 [6, 5376, 16, 128], replicated
- wo: bfloat16 [6, 32, 128, 5376], replicated
Outputs:
- output: bfloat16 [4096, 5376], P(('dp', 'cp')), parts along dimension 0
There are 2 independent parts. The reference program is written for one: setup_inputs(seed, part) draws one part's arguments, and reference() takes and returns one part's arrays. A program takes and returns all parts, laid end to end along the dimension named above; an argument that names none is the same for every part.
All inputs are finite; a program needn't handle non-finite values.
Results may differ from the reference program's by a relative error of at most 0.0118365.
Values are sent between devices in bfloat16 or wider.
A program may use at most 3 GiB of HBM per device.

```python
import jax
import jax.numpy as jnp
from jax import lax

SEQ = 2048
D = 5376
HEADS = 32
KV_HEADS = 16
HEAD = 128
WINDOW = 1024
LAYERS = 6


def setup_inputs(seed: int = 0, part: int = 0) -> dict:
    base = jax.random.key(seed)
    kz, km = jax.random.split(jax.random.fold_in(base, part))
    nseg = 32
    means = jax.random.normal(km, (nseg, D), jnp.float32)
    x = jax.random.normal(kz, (SEQ, D), jnp.float32) + jnp.repeat(means, SEQ // nseg, axis=0)
    kq, kk, kv, ko = jax.random.split(jax.random.key(seed + 1), 4)
    wq = jax.random.normal(kq, (LAYERS, D, HEADS, HEAD), jnp.float32) * D ** -0.5
    wk = jax.random.normal(kk, (LAYERS, D, KV_HEADS, HEAD), jnp.float32) * D ** -0.5
    wv = jax.random.normal(kv, (LAYERS, D, KV_HEADS, HEAD), jnp.float32) * D ** -0.5
    wo = jax.random.normal(ko, (LAYERS, HEADS, HEAD, D), jnp.float32) * (2.0 * (HEADS * HEAD) ** -0.5)
    return {'x': x.astype(jnp.bfloat16), 'wq': wq.astype(jnp.bfloat16), 'wk': wk.astype(jnp.bfloat16), 'wv': wv.astype(jnp.bfloat16), 'wo': wo.astype(jnp.bfloat16)}


def rms_norm(x):
    xf = x.astype(jnp.float32)
    return (xf * lax.rsqrt(jnp.mean(xf * xf, axis=-1, keepdims=True) + 1e-6)).astype(jnp.bfloat16)


def attend(q, k, v, local):
    group = HEADS // KV_HEADS
    qb = min(SEQ, 64)
    nb = SEQ // qb
    scale = HEAD ** -0.5
    qf = q.astype(jnp.float32).reshape(nb, qb, KV_HEADS, group, HEAD)
    kf = k.astype(jnp.float32).reshape(SEQ, KV_HEADS, HEAD)
    vf = v.astype(jnp.float32).reshape(SEQ, KV_HEADS, HEAD)
    if local:
        kf = jnp.pad(kf, ((WINDOW, 0), (0, 0), (0, 0)))
        vf = jnp.pad(vf, ((WINDOW, 0), (0, 0), (0, 0)))
        span = WINDOW + qb
        lead = WINDOW
        reach = WINDOW
        stride = qb
    else:
        span = SEQ
        lead = 0
        reach = SEQ + 1
        stride = 0

    def block(args):
        b, qblk = args
        start = b * stride
        ks = lax.dynamic_slice_in_dim(kf, start, span, axis=0)
        vs = lax.dynamic_slice_in_dim(vf, start, span, axis=0)
        kpos = start - lead + jnp.arange(span)
        qpos = b * qb + jnp.arange(qb)
        s = jnp.einsum('qhgd,khd->qhgk', qblk, ks) * scale
        mask = (kpos[None, :] >= 0) & (kpos[None, :] <= qpos[:, None]) & (kpos[None, :] > qpos[:, None] - reach)
        s = jnp.where(mask[:, None, None, :], s, -jnp.inf)
        p = jax.nn.softmax(s, axis=-1)
        return jnp.einsum('qhgk,khd->qhgd', p, vs)

    o = lax.map(block, (jnp.arange(nb), qf))
    return o.reshape(SEQ, HEADS * HEAD).astype(jnp.bfloat16)


def layer(x, wq_l, wk_l, wv_l, wo_l, local):
    h = rms_norm(x)
    q = jnp.dot(h, wq_l.reshape(D, HEADS * HEAD), preferred_element_type=jnp.float32).astype(jnp.bfloat16)
    k = jnp.dot(h, wk_l.reshape(D, KV_HEADS * HEAD), preferred_element_type=jnp.float32).astype(jnp.bfloat16)
    v = jnp.dot(h, wv_l.reshape(D, KV_HEADS * HEAD), preferred_element_type=jnp.float32).astype(jnp.bfloat16)
    o = attend(q, k, v, local)
    y = jnp.dot(o, wo_l.reshape(HEADS * HEAD, D), preferred_element_type=jnp.float32)
    return (x.astype(jnp.float32) + y).astype(jnp.bfloat16)


def reference(x, wq, wk, wv, wo):
    nloc = LAYERS - 1

    def step(xc, w):
        return layer(xc, w[0], w[1], w[2], w[3], True), None

    x, _ = lax.scan(step, x, (wq[:nloc], wk[:nloc], wv[:nloc], wo[:nloc]))
    return layer(x, wq[nloc], wk[nloc], wv[nloc], wo[nloc], False)
```

```python
import functools
import jax
import jax.numpy as jnp
from jax import lax
from jax.experimental import pallas as pl
from jax.experimental.pallas import tpu as pltpu
from jax.sharding import PartitionSpec as P

F32 = jnp.float32
BF16 = jnp.bfloat16
LAYERS, D, HEADS, KVH, HD = 6, 5376, 32, 16, 128
T = 256
PT = 2 * T
QB = 256
KC = 1792
KS = 256
WN = 768
NW = D // WN
WSLOTS = 3
CW = 1024
G = 2
GW = CW // G
HPG = 8 // G
NEG = -1e30
CSCALE = (HD ** -0.5) * 1.4426950408889634
PIECES = [(t, g) for g in range(G) for t in (0, 1)]


def kernel(x_hbm, wq, wk, wv, wo, out, x, h, kv, q, orecv, acc, wa, wb, m_s, l_s, a_s,
           sx, swa, swb, hs, hr, osd, orv, ks, kr, so, credit):
    r = lax.axis_index('cp')
    c = r // 2
    k = r % 2
    mate = r + 1 - 2 * k
    own = pl.multiple_of(k * T, T)
    oth = pl.multiple_of((1 - k) * T, T)
    row0 = pl.multiple_of(c * PT, PT)

    barrier = pltpu.get_barrier_semaphore()
    for d in range(1, 8):
        pl.semaphore_signal(barrier, inc=1, device_id={'cp': (r + d) % 8})
    pl.semaphore_wait(barrier, 7)

    def wa_copy(l, g, kc, which):
        rows = pl.ds(kc * KC, KC)
        if which == 0:
            src = wk.at[l, rows, pl.ds(pl.multiple_of(k * 8, 8), 8), :]
        elif which == 1:
            src = wv.at[l, rows, pl.ds(pl.multiple_of(k * 8, 8), 8), :]
        else:
            src = wq.at[l, rows, pl.ds(pl.multiple_of(k * 16 + (g - 2) * 8, 8), 8), :]
        return pltpu.make_async_copy(src, wa.at[kc], swa.at[kc])

    def wa_start(l, g, kc):
        @pl.when(g == 0)
        def _():
            wa_copy(l, g, kc, 0).start()

        @pl.when(g == 1)
        def _():
            wa_copy(l, g, kc, 1).start()

        @pl.when(g >= 2)
        def _():
            wa_copy(l, g, kc, 2).start()

    def wb_copy(l, n, slot):
        cols = pl.ds(pl.multiple_of(n * WN, WN), WN)
        return pltpu.make_async_copy(wo.at[l, :, :, cols], wb.at[slot], swb.at[slot])

    xin = pltpu.make_async_copy(x_hbm, x, sx)
    xin.start()
    for kc in range(3):
        wa_copy(0, 0, kc, 0).start()
    for n in range(WSLOTS):
        wb_copy(0, n, n).start()
    xin.wait()

    def x_send(n):
        cols = pl.ds(pl.multiple_of(n * WN, WN), WN)
        return pltpu.make_async_remote_copy(x.at[:, cols], h.at[pl.ds(own, T), cols], hs.at[n], hr.at[n],
                                            device_id={'cp': mate})

    def o_send(p):
        cols = pl.ds(p * 1024, 1024)
        return pltpu.make_async_remote_copy(q.at[pl.ds(oth, T), cols], orecv.at[:, cols], osd.at[p], orv.at[p],
                                            device_id={'cp': mate})

    def kv_copy(par, t, g, slot, chip, idx):
        piece = kv.at[par, t, pl.ds(pl.multiple_of(slot * PT, PT), PT), pl.ds(g * GW, GW)]
        return pltpu.make_async_remote_copy(piece, piece, ks.at[par, t, g, idx], kr.at[par, t, g, slot],
                                            device_id={'cp': 2 * chip + k})

    def kv_sends(l, par, t, g, act):
        @pl.when(c == 0)
        def _():
            act(kv_copy(par, t, g, 0, 1, 0))
            act(kv_copy(par, t, g, 0, 2, 1))

        @pl.when((c == 0) & (l == LAYERS - 1))
        def _():
            act(kv_copy(par, t, g, 0, 3, 2))

        @pl.when((c == 1) | (c == 2))
        def _():
            act(kv_copy(par, t, g, c, 3, 0))

    def start(cp):
        cp.start()

    def wait_send(cp):
        cp.wait_send()

    def kv_wait_recv(par, t, g, slot):
        kv_copy(par, t, g, slot, c, 0).wait_recv()

    def credits_wait():
        @pl.when(c <= 2)
        def _():
            pl.semaphore_wait(credit.at[0], 1)

        @pl.when(c == 0)
        def _():
            pl.semaphore_wait(credit.at[1], 1)

    def credits_give():
        def give(chip, idx):
            pl.semaphore_signal(credit.at[idx], inc=1, device_id={'cp': 2 * chip + k})

        @pl.when(c == 1)
        def _():
            give(0, 0)

        @pl.when(c == 2)
        def _():
            give(0, 1)
            give(3, 1)

        @pl.when(c == 3)
        def _():
            give(1, 0)
            give(2, 0)

    def relay(l, t, g, first):
        par = l % 2

        @pl.when((c == 3) & (l < LAYERS))
        def _():
            if first:
                @pl.when(l >= 2)
                def _():
                    pl.semaphore_wait(credit.at[1], 1)
            kv_wait_recv(par, t, g, 1)
            kv_copy(par, t, g, 1, 2, 1).start()

    def relay_wait(l):
        par = l % 2

        @pl.when(c == 3)
        def _():
            for t, g in PIECES:
                kv_copy(par, t, g, 1, 2, 1).wait_send()

    rowi = lax.broadcasted_iota(jnp.int32, (2 * QB, QB), 0) % QB
    coli = lax.broadcasted_iota(jnp.int32, (2 * QB, QB), 1)

    def tile(par, j, b, kb, mode, first):
        jq = pl.multiple_of(j * 256, 256)
        rows = pl.ds(b * QB, QB)
        kcols = pl.ds(pl.multiple_of(j * HD, HD), HD)
        krows = pl.ds(pl.multiple_of(kb * QB, QB), QB)
        qq = jnp.concatenate([q[rows, pl.ds(jq, HD)], q[rows, pl.ds(pl.multiple_of(jq + HD, HD), HD)]], axis=0)
        s = lax.dot_general(qq, kv[par, 0, krows, kcols], (((1,), (1,)), ((), ())), preferred_element_type=F32)
        s = s * CSCALE
        if mode == 'diag':
            s = jnp.where(coli <= rowi, s, NEG)
        elif mode == 'old':
            s = jnp.where(coli > rowi, s, NEG)
        mx = jnp.max(s, axis=1, keepdims=True)
        v = kv[par, 1, krows, kcols]
        if first:
            mn = jnp.broadcast_to(mx, (2 * QB, HD))
            p = jnp.exp2(s - jnp.concatenate([mn, mn], axis=1))
            l_s[b] = p[:, :HD] + p[:, HD:]
            a_s[b] = jnp.dot(p.astype(BF16), v, preferred_element_type=F32)
        else:
            mo = m_s[b]
            mn = jnp.maximum(mo, mx)
            p = jnp.exp2(s - jnp.concatenate([mn, mn], axis=1))
            al = jnp.exp2(mo - mn)
            l_s[b] = l_s[b] * al + (p[:, :HD] + p[:, HD:])
            a_s[b] = a_s[b] * al + jnp.dot(p.astype(BF16), v, preferred_element_type=F32)
        m_s[b] = mn

    def attention(l, par):
        last = l == LAYERS - 1

        def head(j, _):
            @pl.when(j % HPG == 0)
            def _():
                g = j // HPG
                for s in range(3):
                    @pl.when((s < c) & ((s >= c - 2) | last) & ((c != 3) | (s != 1)))
                    def _():
                        for t in (0, 1):
                            kv_dyn_wait(par, t, g, s)
            for b in (0, 1):
                tile(par, j, b, 2 * c + b, 'diag', True)
            hi = jnp.where(last, 2 * c, jnp.minimum(3, 2 * c))

            def mid(t, _):
                for b in (0, 1):
                    tile(par, j, b, 2 * c + b - t, 'mid', False)
                return 0

            lax.fori_loop(1, hi + 1, mid, 0)

            @pl.when(last | (c <= 1))
            def _():
                tile(par, j, 1, 0, 'mid', False)

            @pl.when((c >= 2) & jnp.logical_not(last))
            def _():
                for b in (0, 1):
                    tile(par, j, b, 2 * c + b - 4, 'old', False)
            jq = pl.multiple_of(j * 256, 256)
            for b in (0, 1):
                o = a_s[b] / jnp.sum(l_s[b], axis=1, keepdims=True)
                o = o.astype(BF16)
                q[b * QB:(b + 1) * QB, pl.ds(jq, HD)] = o[:QB]
                q[b * QB:(b + 1) * QB, pl.ds(pl.multiple_of(jq + HD, HD), HD)] = o[QB:]

            @pl.when(j == 4)
            def _():
                o_send(0).start()
            return 0

        lax.fori_loop(0, 8, head, 0)
        o_send(1).start()

    def kv_dyn_wait(par, t, g, slot):
        piece = kv.at[par, t, pl.ds(slot * PT, PT), pl.ds(pl.multiple_of(g * GW, GW), GW)]
        pltpu.make_async_remote_copy(piece, piece, ks.at[par, t, g, 0], kr.at[par, t, g, slot],
                                     device_id={'cp': mate}).wait_recv()

    def norm_rows(src, dst, r0):
        def blk(i, _):
            rows = pl.ds(pl.multiple_of(r0 + i * 16, 16), 16)
            srows = rows if src is h else pl.ds(pl.multiple_of(i * 16, 16), 16)
            xf = src[srows, :].astype(F32)
            ms = jnp.mean(xf * xf, axis=-1, keepdims=True)
            dst[rows, :] = (xf * lax.rsqrt(ms + 1e-6)).astype(BF16)
            return 0
        lax.fori_loop(0, T // 16, blk, 0)

    for n in range(NW):
        x_send(n).start()

    def layer(l, _):
        par = l % 2
        norm_rows(x, h, own)
        for n in range(NW):
            x_send(n).wait()
        norm_rows(h, h, oth)

        @pl.when(l >= 2)
        def _():
            for t, g in PIECES:
                kv_sends(l - 2, par, t, g, wait_send)
            credits_wait()

        def group(g, _):
            for kc in range(3):
                wa_copy(l, g, kc, 0).wait()
                for s in range(KC // KS):
                    w = wa[kc, s * KS:(s + 1) * KS].reshape(KS, CW)
                    o = kc * KC + s * KS
                    p = jnp.dot(h[:, o:o + KS], w, preferred_element_type=F32)
                    if o == 0:
                        acc[...] = p
                    else:
                        acc[...] += p

                @pl.when(g < 3)
                def _():
                    wa_start(l, g + 1, kc)

                @pl.when((g == 3) & (l < LAYERS - 1))
                def _():
                    wa_copy(l + 1, 0, kc, 0).start()

                if kc == 0:
                    @pl.when(g == 1)
                    def _():
                        kv_sends(l, par, 0, 0, start)

                    @pl.when(g == 2)
                    def _():
                        kv_sends(l, par, 1, 0, start)
                        for gg in range(1, G):
                            kv_sends(l, par, 0, gg, start)
                            kv_sends(l, par, 1, gg, start)

            @pl.when(g == 0)
            def _():
                kv[par, 0, pl.ds(row0, PT), :] = acc[...].astype(BF16)

            @pl.when(g == 1)
            def _():
                kv[par, 1, pl.ds(row0, PT), :] = acc[...].astype(BF16)

            @pl.when(g >= 2)
            def _():
                q[:, pl.ds(pl.multiple_of((g - 2) * CW, CW), CW)] = acc[...].astype(BF16)

            @pl.when((g == 0) & (l >= 1))
            def _():
                relay(l, 1, 1, False)
            return 0

        @pl.when(l >= 1)
        def _():
            for p in range(2):
                o_send(p).wait_send()
        lax.fori_loop(0, 4, group, 0)

        @pl.when(l == 0)
        def _():
            for i, (t, g) in enumerate(PIECES):
                relay(l, t, g, i == 0)
        relay(l + 1, 0, 0, True)

        attention(l, par)
        relay_wait(l)

        @pl.when(l <= LAYERS - 3)
        def _():
            credits_give()
        relay(l + 1, 1, 0, False)
        for p in range(2):
            o_send(p).wait_recv()

        def chunk(n, _):
            slot = (l * NW + n) % WSLOTS
            wb_copy(l, n, slot).wait()
            cols = pl.ds(pl.multiple_of(n * WN, WN), WN)
            wown = wb[slot, pl.ds(k * 16, 16)].reshape(2048, WN)
            woth = wb[slot, pl.ds((1 - k) * 16, 16)].reshape(2048, WN)
            y = jnp.dot(q[pl.ds(own, T), :], wown, preferred_element_type=F32)
            y = y + jnp.dot(orecv[...], woth, preferred_element_type=F32)
            x[:, cols] = (x[:, cols].astype(F32) + y).astype(BF16)

            @pl.when(n + WSLOTS < NW)
            def _():
                wb_copy(l, n + WSLOTS, slot).start()

            @pl.when((n + WSLOTS >= NW) & (l < LAYERS - 1))
            def _():
                wb_copy(l + 1, n + WSLOTS - NW, slot).start()

            @pl.when((n > 0) & (l < LAYERS - 1))
            def _():
                x_send(n - 1).start()
            return 0

        lax.fori_loop(0, NW, chunk, 0)

        @pl.when(l < LAYERS - 1)
        def _():
            x_send(NW - 1).start()
        relay(l + 1, 0, 1, False)
        return 0

    lax.fori_loop(0, LAYERS, layer, 0)

    res = pltpu.make_async_copy(x, out, so)
    res.start()
    for p in range(2):
        o_send(p).wait_send()
    for l in (LAYERS - 2, LAYERS - 1):
        for t, g in PIECES:
            kv_sends(l, l % 2, t, g, wait_send)
    res.wait()


def solution(mesh):
    def body(x, wq, wk, wv, wo):
        anyspec = pl.BlockSpec(memory_space=pl.ANY)
        dma = pltpu.SemaphoreType.DMA
        return pl.pallas_call(
            kernel,
            out_shape=jax.ShapeDtypeStruct((T, D), BF16),
            in_specs=[anyspec] * 5,
            out_specs=anyspec,
            scratch_shapes=[
                pltpu.VMEM((T, D), BF16),
                pltpu.VMEM((PT, D), BF16),
                pltpu.VMEM((2, 2, 4 * PT, CW), BF16),
                pltpu.VMEM((PT, 2048), BF16),
                pltpu.VMEM((T, 2048), BF16),
                pltpu.VMEM((PT, CW), F32),
                pltpu.VMEM((3, KC, 8, HD), BF16),
                pltpu.VMEM((WSLOTS, HEADS, HD, WN), BF16),
                pltpu.VMEM((2, PT, HD), F32),
                pltpu.VMEM((2, PT, HD), F32),
                pltpu.VMEM((2, PT, HD), F32),
                dma, dma((3,)), dma((WSLOTS,)), dma((NW,)), dma((NW,)), dma((2,)), dma((2,)),
                dma((2, 2, G, 3)), dma((2, 2, G, 4)), dma,
                pltpu.SemaphoreType.REGULAR((2,)),
            ],
            compiler_params=pltpu.CompilerParams(collective_id=0, has_side_effects=True,
                                                 vmem_limit_bytes=67043328),
            cost_estimate=pl.CostEstimate(flops=240 * 10 ** 9, bytes_accessed=530 * 10 ** 6, transcendentals=0),
        )(x, wq, wk, wv, wo)

    spec_x = P(('dp', 'cp'), None)
    return jax.shard_map(body, mesh=mesh, in_specs=(spec_x, P(), P(), P(), P()), out_specs=spec_x, check_vma=False)
```

```python
import functools
import jax
import jax.numpy as jnp
from jax import lax
from jax.experimental import pallas as pl
from jax.experimental.pallas import tpu as pltpu
from jax.sharding import PartitionSpec as P

F32 = jnp.float32
BF16 = jnp.bfloat16
LAYERS, D, HEADS, KVH, HD = 6, 5376, 32, 16, 128
T = 256
PT = 2 * T
QB = 256
KC = 1792
KS = 256
WN = 768
NW = D // WN
WSLOTS = 3
CW = 1024
G = 4
GW = CW // G
HPG = 8 // G
NEG = -1e30
CSCALE = (HD ** -0.5) * 1.4426950408889634
PIECES = [(0, 0), (0, 1), (1, 0), (1, 1), (0, 2), (1, 2), (0, 3), (1, 3)]


def kernel(x_hbm, wq, wk, wv, wo, out, x, h, kb_, vb_, q, orecv, acc, wa, wb, m_s, l_s, a_s, s_s,
           sx, swa, swb, hs, hr, osd, orv, ks, kr, so, credit):
    r = lax.axis_index('cp')
    c = r // 2
    k = r % 2
    mate = r + 1 - 2 * k
    own = pl.multiple_of(k * T, T)
    oth = pl.multiple_of((1 - k) * T, T)
    row0 = pl.multiple_of(c * PT, PT)

    barrier = pltpu.get_barrier_semaphore()
    for d in range(1, 8):
        pl.semaphore_signal(barrier, inc=1, device_id={'cp': (r + d) % 8})
    pl.semaphore_wait(barrier, 7)

    def wa_copy(l, g, kc, which):
        rows = pl.ds(kc * KC, KC)
        if which == 0:
            src = wk.at[l, rows, pl.ds(pl.multiple_of(k * 8, 8), 8), :]
        elif which == 1:
            src = wv.at[l, rows, pl.ds(pl.multiple_of(k * 8, 8), 8), :]
        else:
            src = wq.at[l, rows, pl.ds(pl.multiple_of(k * 16 + (g - 2) * 8, 8), 8), :]
        return pltpu.make_async_copy(src, wa.at[kc], swa.at[kc])

    def wa_start(l, g, kc):
        @pl.when(g == 0)
        def _():
            wa_copy(l, g, kc, 0).start()

        @pl.when(g == 1)
        def _():
            wa_copy(l, g, kc, 1).start()

        @pl.when(g >= 2)
        def _():
            wa_copy(l, g, kc, 2).start()

    def wb_copy(l, n, slot):
        cols = pl.ds(pl.multiple_of(n * WN, WN), WN)
        return pltpu.make_async_copy(wo.at[l, :, :, cols], wb.at[slot], swb.at[slot])

    xin = pltpu.make_async_copy(x_hbm, x, sx)
    xin.start()
    for kc in range(3):
        wa_copy(0, 0, kc, 0).start()
    for n in range(WSLOTS):
        wb_copy(0, n, n).start()
    xin.wait()

    def x_send(n):
        cols = pl.ds(pl.multiple_of(n * WN, WN), WN)
        return pltpu.make_async_remote_copy(x.at[:, cols], h.at[pl.ds(own, T), cols], hs.at[n], hr.at[n],
                                            device_id={'cp': mate})

    def o_send(p):
        cols = pl.ds(p * 1024, 1024)
        return pltpu.make_async_remote_copy(q.at[pl.ds(oth, T), cols], orecv.at[:, cols], osd.at[p], orv.at[p],
                                            device_id={'cp': mate})

    def kv_piece(par, t, g, slot):
        if t == 0:
            return kb_.at[par, g, pl.ds(pl.multiple_of(slot * PT, PT), PT), :]
        return vb_.at[par, slot, pl.ds(pl.multiple_of(g * GW, GW), GW), :]

    def kv_copy(par, t, g, slot, chip, idx):
        piece = kv_piece(par, t, g, slot)
        return pltpu.make_async_remote_copy(piece, piece, ks.at[par, t, g, idx], kr.at[par, t, g, slot],
                                            device_id={'cp': 2 * chip + k})

    def kv_sends(l, par, t, g, act):
        @pl.when(c == 0)
        def _():
            act(kv_copy(par, t, g, 0, 1, 0))
            act(kv_copy(par, t, g, 0, 2, 1))

        @pl.when((c == 1) | (c == 2))
        def _():
            act(kv_copy(par, t, g, c, 3, 0))

    def kv_far(par, t, g):
        return kv_copy(par, t, g, 0, 3, 2)

    def start(cp):
        cp.start()

    def wait_send(cp):
        cp.wait_send()

    def kv_wait_recv(par, t, g, slot):
        kv_copy(par, t, g, slot, c, 0).wait_recv()

    def credits_wait():
        @pl.when(c <= 2)
        def _():
            pl.semaphore_wait(credit.at[0], 1)

        @pl.when(c == 0)
        def _():
            pl.semaphore_wait(credit.at[1], 1)

    def credits_give():
        def give(chip, idx):
            pl.semaphore_signal(credit.at[idx], inc=1, device_id={'cp': 2 * chip + k})

        @pl.when(c == 1)
        def _():
            give(0, 0)

        @pl.when(c == 2)
        def _():
            give(0, 1)
            give(3, 1)

        @pl.when(c == 3)
        def _():
            give(1, 0)
            give(2, 0)

    def relay(l, t, g):
        par = l % 2

        @pl.when((c == 3) & (l < LAYERS))
        def _():
            if (t, g) == PIECES[0]:
                @pl.when(l >= 2)
                def _():
                    pl.semaphore_wait(credit.at[1], 1)
            kv_wait_recv(par, t, g, 1)
            kv_copy(par, t, g, 1, 2, 1).start()

    def relay_wait(l):
        par = l % 2

        @pl.when(c == 3)
        def _():
            for t, g in PIECES:
                kv_copy(par, t, g, 1, 2, 1).wait_send()

    keyi = lax.broadcasted_iota(jnp.int32, (QB, 2 * QB), 0)
    qryi = lax.broadcasted_iota(jnp.int32, (QB, 2 * QB), 1) % QB

    def score(par, j, b, kb, mode, slot):
        jq = pl.multiple_of(j * 256, 256)
        rows = pl.ds(b * QB, QB)
        kcols = pl.ds(pl.multiple_of((j % HPG) * HD, HD), HD)
        krows = pl.ds(pl.multiple_of(kb * QB, QB), QB)
        qq = jnp.concatenate([q[rows, pl.ds(jq, HD)], q[rows, pl.ds(pl.multiple_of(jq + HD, HD), HD)]], axis=0)
        s = lax.dot_general(kb_[par, j // HPG, krows, kcols], qq, (((1,), (1,)), ((), ())), preferred_element_type=F32)
        s = s * CSCALE
        if mode == 'diag':
            s = jnp.where(keyi <= qryi, s, NEG)
        elif mode == 'old':
            s = jnp.where(keyi > qryi, s, NEG)
        s_s[slot] = s
        return jnp.max(s, axis=0, keepdims=True)

    def consume(par, j, b, kb, mx, slot, first):
        kcols = pl.ds(pl.multiple_of(j * HD, HD), HD)
        v = vb_[par, kb // 2, kcols, pl.ds(pl.multiple_of((kb % 2) * QB, QB), QB)]
        if first:
            p = jnp.exp2(s_s[slot] - mx)
            l_s[b] = jnp.sum(p, axis=0, keepdims=True)
            a_s[b] = jnp.dot(v, p.astype(BF16), preferred_element_type=F32)
            m_s[b] = mx
        else:
            mo = m_s[b]
            mn = jnp.maximum(mo, mx)
            p = jnp.exp2(s_s[slot] - mn)
            al = jnp.exp2(mo - mn)
            l_s[b] = l_s[b] * al + jnp.sum(p, axis=0, keepdims=True)
            a_s[b] = a_s[b] * al + jnp.dot(v, p.astype(BF16), preferred_element_type=F32)
            m_s[b] = mn

    def tiles(par, j, items):
        mx = None
        for i in range(len(items) + 1):
            nxt = None
            if i < len(items):
                b, kb, mode, first = items[i]
                nxt = score(par, j, b, kb, mode, i % 2)
            if i > 0:
                b, kb, mode, first = items[i - 1]
                consume(par, j, b, kb, mx, (i - 1) % 2, first)
            mx = nxt

    def attention(l, par):
        last = l == LAYERS - 1

        def head(j, _):
            @pl.when(j % HPG == 0)
            def _():
                g = j // HPG
                for s in range(3):
                    @pl.when((s < c) & ((s >= c - 2) | last) & ((c != 3) | (s != 1))
                             & ((c != 2) | (s != 0) | jnp.logical_not(last) | (g >= 2)))
                    def _():
                        for t in (0, 1):
                            kv_dyn_wait(par, t, g, s)
            full = (c >= 2) & jnp.logical_not(last)

            @pl.when(full)
            def _():
                tiles(par, j, [(b, 2 * c + b - t, ('diag', 'mid', 'mid', 'mid', 'old')[t], t == 0)
                               for t in range(5) for b in (0, 1)])

            @pl.when(jnp.logical_not(full))
            def _():
                tiles(par, j, [(b, 2 * c + b, 'diag', True) for b in (0, 1)])

                def mid(i, _):
                    tiles(par, j, [(b, 2 * c + b - 1 - 2 * i - u, 'mid', False) for u in (0, 1) for b in (0, 1)])
                    return 0

                lax.fori_loop(0, c, mid, 0)
                tiles(par, j, [(1, 0, 'mid', False)])

            jq = pl.multiple_of(j * 256, 256)
            for b in (0, 1):
                o = (a_s[b] * (1.0 / l_s[b])).T.astype(BF16)
                q[b * QB:(b + 1) * QB, pl.ds(jq, HD)] = o[:QB]
                q[b * QB:(b + 1) * QB, pl.ds(pl.multiple_of(jq + HD, HD), HD)] = o[QB:]

            @pl.when(j == 4)
            def _():
                o_send(0).start()
            return 0

        lax.fori_loop(0, 8, head, 0)
        o_send(1).start()

    def kv_dyn_wait(par, t, g, slot):
        piece = kv_piece(par, t, g, slot)
        pltpu.make_async_remote_copy(piece, piece, ks.at[par, t, g, 0], kr.at[par, t, g, slot],
                                     device_id={'cp': mate}).wait_recv()

    def norm_rows(src, dst, r0):
        def blk(i, _):
            rows = pl.ds(pl.multiple_of(r0 + i * 16, 16), 16)
            srows = rows if src is h else pl.ds(pl.multiple_of(i * 16, 16), 16)
            xf = src[srows, :].astype(F32)
            ms = jnp.mean(xf * xf, axis=-1, keepdims=True)
            dst[rows, :] = (xf * lax.rsqrt(ms + 1e-6)).astype(BF16)
            return 0
        lax.fori_loop(0, T // 16, blk, 0)

    for n in range(NW):
        x_send(n).start()

    def layer(l, _):
        par = l % 2
        norm_rows(x, h, own)
        for n in range(NW):
            x_send(n).wait()
        norm_rows(h, h, oth)

        @pl.when(l >= 1)
        def _():
            relay(l, *PIECES[4])

        @pl.when(l >= 2)
        def _():
            for t, g in PIECES:
                kv_sends(l - 2, par, t, g, wait_send)
            credits_wait()

        def group(g, _):
            for kc in range(3):
                wa_copy(l, g, kc, 0).wait()
                for s in range(KC // KS):
                    w = wa[kc, s * KS:(s + 1) * KS].reshape(KS, CW)
                    o = kc * KC + s * KS
                    p = jnp.dot(h[:, o:o + KS], w, preferred_element_type=F32)
                    if o == 0:
                        acc[...] = p
                    else:
                        acc[...] += p

                @pl.when(g < 3)
                def _():
                    wa_start(l, g + 1, kc)

                @pl.when((g == 3) & (l < LAYERS - 1))
                def _():
                    wa_copy(l + 1, 0, kc, 0).start()

                if kc == 0:
                    @pl.when(g == 1)
                    def _():
                        for t, gg in PIECES[:2]:
                            kv_sends(l, par, t, gg, start)

                    @pl.when(g == 2)
                    def _():
                        for t, gg in PIECES[2:]:
                            kv_sends(l, par, t, gg, start)

                    @pl.when((g == 1) & (l >= 1))
                    def _():
                        relay(l, *PIECES[6])

            @pl.when(g == 0)
            def _():
                for gg in range(G):
                    kb_[par, gg, pl.ds(row0, PT), :] = acc[:, gg * GW:(gg + 1) * GW].astype(BF16)

            @pl.when(g == 1)
            def _():
                vb_[par, c] = acc[...].T.astype(BF16)

            @pl.when(g >= 2)
            def _():
                q[:, pl.ds(pl.multiple_of((g - 2) * CW, CW), CW)] = acc[...].astype(BF16)

            @pl.when((g == 0) & (l >= 1))
            def _():
                relay(l, *PIECES[5])

            @pl.when((g == 1) & (l >= 1))
            def _():
                relay(l, *PIECES[7])
            return 0

        @pl.when(l >= 1)
        def _():
            for p in range(2):
                o_send(p).wait_send()
        lax.fori_loop(0, 4, group, 0)

        @pl.when(l == 0)
        def _():
            for t, g in PIECES:
                relay(l, t, g)

        attention(l, par)
        relay_wait(l)

        @pl.when(l <= LAYERS - 3)
        def _():
            credits_give()
        for p in range(2):
            o_send(p).wait_recv()

        def chunk(n, _):
            slot = (l * NW + n) % WSLOTS
            for i, at in enumerate((0, 3, 5)):
                @pl.when(n == at)
                def _():
                    relay(l + 1, *PIECES[i])

            @pl.when((c == 2) & (n == 3) & (l == LAYERS - 2))
            def _():
                for t, g in PIECES[:4]:
                    kv_wait_recv((LAYERS - 1) % 2, t, g, 0)
                    kv_copy((LAYERS - 1) % 2, t, g, 0, 3, 1).start()

            wb_copy(l, n, slot).wait()
            cols = pl.ds(pl.multiple_of(n * WN, WN), WN)
            wown = wb[slot, pl.ds(k * 16, 16)].reshape(2048, WN)
            woth = wb[slot, pl.ds((1 - k) * 16, 16)].reshape(2048, WN)
            y = jnp.dot(q[pl.ds(own, T), :], wown, preferred_element_type=F32)
            y = y + jnp.dot(orecv[...], woth, preferred_element_type=F32)
            x[:, cols] = (x[:, cols].astype(F32) + y).astype(BF16)

            @pl.when(n + WSLOTS < NW)
            def _():
                wb_copy(l, n + WSLOTS, slot).start()

            @pl.when((n + WSLOTS >= NW) & (l < LAYERS - 1))
            def _():
                wb_copy(l + 1, n + WSLOTS - NW, slot).start()

            @pl.when((n > 0) & (l < LAYERS - 1))
            def _():
                x_send(n - 1).start()
            return 0

        lax.fori_loop(0, NW, chunk, 0)

        @pl.when(l < LAYERS - 1)
        def _():
            x_send(NW - 1).start()
        relay(l + 1, *PIECES[3])
        return 0

    lax.fori_loop(0, LAYERS, layer, 0)

    res = pltpu.make_async_copy(x, out, so)
    res.start()
    for p in range(2):
        o_send(p).wait_send()
    for l in (LAYERS - 2, LAYERS - 1):
        for t, g in PIECES:
            kv_sends(l, l % 2, t, g, wait_send)

    @pl.when(c == 0)
    def _():
        for t, g in PIECES[4:]:
            kv_far((LAYERS - 1) % 2, t, g).start()
        for t, g in PIECES[4:]:
            kv_far((LAYERS - 1) % 2, t, g).wait_send()

    @pl.when(c == 2)
    def _():
        for t, g in PIECES[:4]:
            kv_copy((LAYERS - 1) % 2, t, g, 0, 3, 1).wait_send()
    res.wait()


def solution(mesh):
    def body(x, wq, wk, wv, wo):
        anyspec = pl.BlockSpec(memory_space=pl.ANY)
        dma = pltpu.SemaphoreType.DMA
        return pl.pallas_call(
            kernel,
            out_shape=jax.ShapeDtypeStruct((T, D), BF16),
            in_specs=[anyspec] * 5,
            out_specs=anyspec,
            scratch_shapes=[
                pltpu.VMEM((T, D), BF16),
                pltpu.VMEM((PT, D), BF16),
                pltpu.VMEM((2, G, 4 * PT, GW), BF16),
                pltpu.VMEM((2, 4, CW, PT), BF16),
                pltpu.VMEM((PT, 2048), BF16),
                pltpu.VMEM((T, 2048), BF16),
                pltpu.VMEM((PT, CW), F32),
                pltpu.VMEM((3, KC, 8, HD), BF16),
                pltpu.VMEM((WSLOTS, HEADS, HD, WN), BF16),
                pltpu.VMEM((2, 1, 2 * QB), F32),
                pltpu.VMEM((2, 1, 2 * QB), F32),
                pltpu.VMEM((2, HD, 2 * QB), F32),
                pltpu.VMEM((2, QB, 2 * QB), F32),
                dma, dma((3,)), dma((WSLOTS,)), dma((NW,)), dma((NW,)), dma((2,)), dma((2,)),
                dma((2, 2, G, 3)), dma((2, 2, G, 4)), dma,
                pltpu.SemaphoreType.REGULAR((2,)),
            ],
            compiler_params=pltpu.CompilerParams(collective_id=0, has_side_effects=True,
                                                 vmem_limit_bytes=67043328),
            cost_estimate=pl.CostEstimate(flops=240 * 10 ** 9, bytes_accessed=530 * 10 ** 6, transcendentals=0),
        )(x, wq, wk, wv, wo)

    spec_x = P(('dp', 'cp'), None)
    return jax.shard_map(body, mesh=mesh, in_specs=(spec_x, P(), P(), P(), P()), out_specs=spec_x, check_vma=False)
```
